32 devices in a mesh: gx: 4 (over z), gy: 4 (over x, core), gz: 2 (over y).
Axes of the slice: x: 2, y: 2, z: 4, core: 2. Of those that a mesh axis runs over, the one named last changes fastest.
Arguments:
- volume: int32 [32, 64, 256], P('gx', 'gy', 'gz'), may hold values from 0 to 255
- transfer_table: float32 [4, 256], replicated, may hold values from 0 to 1
- depth_rank: int32 [4], replicated, may hold values from 0 to 3, each once
- footprint: int32 [4, 4, 2, 4], P('gx', 'gy', 'gz'), may hold values from 0 to 128, as said below
Outputs:
- rendered: float32 [4, 64, 256], P(None, 'gy', 'gz')
The draws below stay inside these ranges and needn't reach their ends.
Inputs may be any that keep to these rules, and one draw needn't show every extreme that they name: depth_rank holds each of 0 to 4 - 1 once. `footprint`: for every brick, entry 0 is below 8 and entry 1 above it, up to 16; entry 2 is below 64 and entry 3 above it, up to 128.
All inputs are finite; a program needn't handle non-finite values.
Results may differ from the reference program's by a relative error of at most 0.0003.
Values sent between devices are 32-bit elements; how exact they have to be, the bound alone decides.
A program may use at most 64 MiB of HBM per device.

```python
import jax
import jax.numpy as jnp
from jax import lax

CX = 8
CY = 16
CZ = 128
TF = 256
NX = 32
NY = 64
NZ = 256
N_GX = 4
N_GY = 4
N_GZ = 2


def draw_footprint(key, part):
    keys = jax.random.split(jax.random.fold_in(key, 7), 4)
    shaped = (N_GX, N_GY, N_GZ)
    first_row = jax.random.randint(keys[0], shaped, 0, CY // 2)
    end_row = jax.random.randint(keys[1], shaped, CY // 2 + 1, CY + 1)
    first_col = jax.random.randint(keys[2], shaped, 0, CZ // 2)
    end_col = jax.random.randint(keys[3], shaped, CZ // 2 + 1, CZ + 1)
    return jnp.stack([first_row, end_row, first_col, end_col], axis=-1).astype(jnp.int32)


def with_ends(result, stream_key, least, high):
    longest = result.shape.index(max(result.shape))
    spots = []
    for shift in (0, 1):
        where = [jax.random.randint(jax.random.fold_in(stream_key, axis), (), 0, length) for axis, length in enumerate(result.shape)]
        where[longest] = (where[longest] + shift) % result.shape[longest]
        spots.append(tuple(where))
    return result.at[spots[0]].set(least).at[spots[1]].set(high)


def setup_inputs(seed: int = 0) -> dict:
    key_list = jax.random.split(jax.random.key(seed), 5)
    return {
        "volume": with_ends(jax.random.randint(key_list[0], (NX, NY, NZ), 0, TF), jax.random.fold_in(key_list[0], 1), 0, TF - 1).astype(jnp.int32),
        "transfer_table": jnp.clip(jax.random.uniform(key_list[1], (4, TF), jnp.float32, 0.0, 1.0), 0.0, 1.0),
        "depth_rank": jax.random.permutation(key_list[2], N_GX).astype(jnp.int32),
        "footprint": draw_footprint(jax.random.fold_in(key_list[4], 71), 0),
    }


light_x = 1.0 / 3.0
light_y = 2.0 / 3.0
light_z = 2.0 / 3.0

def shading(lower_plane, upper_plane, padded):
    grad_x = 0.5 * (upper_plane - lower_plane)
    grad_y = 0.5 * (padded[2:, 1:-1] - padded[:-2, 1:-1])
    grad_z = 0.5 * (padded[1:-1, 2:] - padded[1:-1, :-2])
    facing = jnp.abs(grad_x * light_x + grad_y * light_y + grad_z * light_z) / jnp.sqrt(1.0 + (grad_x * grad_x + grad_y * grad_y + grad_z * grad_z))
    return 0.35 + 0.65 * facing

def composite(layers, depth_rank):
    order = jnp.argsort(depth_rank).astype(jnp.int32)
    ordered = jnp.take(layers, order, axis=0)

    def blend(state_pair, front_layer):
        colour, alpha = state_pair
        cover = 1.0 - alpha
        return ((colour + cover * front_layer[:3], alpha + cover * front_layer[3]), None)
    start_pair = (jnp.zeros((3,) + layers.shape[2:], jnp.float32), jnp.zeros(layers.shape[2:], jnp.float32))
    (colour, alpha), unused = lax.scan(blend, start_pair, ordered)
    return jnp.concatenate([colour, alpha[None]], axis=0)

def reference(volume, transfer_table, depth_rank, footprint):
    opacity = transfer_table[3]
    colors = transfer_table[:3]
    extent = 4.0 / NX

    def density(slice_at):
        inside = ((slice_at >= 0) & (slice_at < NX)).astype(jnp.float32)
        clipped = jnp.clip(slice_at, 0, NX - 1).astype(jnp.int32)
        indices = lax.dynamic_index_in_dim(volume, clipped, 0, keepdims=False)
        return (jnp.take(opacity, indices, axis=0) * inside, indices)

    def advance(state_pair, slice_at):
        colour, transmit = state_pair
        centre, indices = density(slice_at)
        lower_plane, unused_low = density(slice_at - 1)
        upper_plane, unused_high = density(slice_at + 1)
        shading_term = shading(lower_plane, upper_plane, jnp.pad(centre, 1))
        emitted = jnp.take(colors, indices, axis=1) * shading_term
        sample_alpha = 1.0 - jnp.exp(-extent * centre)
        colour = colour + transmit * sample_alpha * emitted
        transmit = transmit * (1.0 - sample_alpha)
        return ((colour, transmit), None)
    rows_local = (jnp.arange(NY, dtype=jnp.int32) % CY)[:, None]
    cols_local = (jnp.arange(NZ, dtype=jnp.int32) % CZ)[None, :]
    partials = []
    for column in range(N_GX):
        start_pair = (jnp.zeros((3, NY, NZ), jnp.float32), jnp.ones((NY, NZ), jnp.float32))
        slices_here = jnp.arange(CX, dtype=jnp.int32) + column * CX
        (colour, transmit), unused = lax.scan(advance, start_pair, slices_here)
        rect = jnp.repeat(jnp.repeat(footprint[column], CY, axis=0), CZ, axis=1)
        inside = (rows_local >= rect[..., 0]) & (rows_local < rect[..., 1]) & (cols_local >= rect[..., 2]) & (cols_local < rect[..., 3])
        layer = jnp.concatenate([colour, (1.0 - transmit)[None]], axis=0)
        partials.append(jnp.where(inside[None], layer, 0.0))
    return composite(jnp.stack(partials), depth_rank)
```

```python
import functools

import jax
import jax.numpy as jnp
from jax import lax
from jax.experimental import pallas as pl
from jax.experimental.pallas import tpu as pltpu
from jax.sharding import PartitionSpec as P

LIGHT = (1.0 / 3.0, 2.0 / 3.0, 2.0 / 3.0)
AXES = ("gx", "gy", "gz")
MESH = pl.DeviceIdType.MESH
RAW = 1


def lookup(table_row, index, lanes):
    entries = table_row.shape[1]
    low = index & (lanes - 1)
    found = None
    for part in range(entries // lanes):
        piece = jnp.broadcast_to(table_row[:, part * lanes:(part + 1) * lanes], index.shape)
        got = jnp.take_along_axis(piece, low, axis=1, mode="promise_in_bounds")
        found = got if found is None else jnp.where(index >= part * lanes, got, found)
    return found


def kernel(sizes, vol_hbm, table_hbm, rank_hbm, foot_hbm, out_ref,
           vols, table_ref, rank_ref, foot_ref, load_sem, frames, yedge, zedge, xh, yh, zh,
           dens, wemit, inner, alphas, colours,
           ready, far_ready, halo_send, halo_recv, front_send, raw_recv, edge_recv, a_send, a_recv, c_send, c_recv):
    n, ny, nz = sizes
    _, depth, rows, lanes = vols.shape
    per = rows // 8
    extent = 4.0 / (depth * n)
    me = [lax.axis_index(a) for a in AXES]
    ix = me[0]
    raw_from = max(1, n - RAW)
    is_raw = ix >= raw_from
    has_lower = [me[a] > 0 for a in range(3)]
    has_upper = [me[a] < sizes[a] - 1 for a in range(3)]

    def signal(sem, **where):
        pl.semaphore_signal(sem, inc=1, device_id=where, device_id_type=MESH)

    barrier = pltpu.get_barrier_semaphore()
    for off in range(n - 1, 0, -1):
        @pl.when(ix + off < n)
        def _():
            signal(barrier, gx=ix + off)
    for a in (1, 2):
        if sizes[a] > 1:
            @pl.when(has_upper[a])
            def _():
                signal(barrier, **{AXES[a]: me[a] + 1})

            @pl.when((ix == 0) & has_upper[a])
            def _():
                for k in range(n - 1, 0, -1):
                    signal(barrier, **{"gx": k, AXES[a]: me[a] + 1})

    loads = [
        pltpu.make_async_copy(src, dst, load_sem.at[i])
        for i, (src, dst) in enumerate((
            (vol_hbm, vols.at[ix]), (table_hbm, table_ref), (foot_hbm, foot_ref), (rank_hbm, rank_ref)
        ))
    ]
    for load in loads:
        load.start()

    greeted = ix
    for a in (1, 2):
        greeted = greeted + lax.min(me[a], 1) * (1 + lax.min(ix, 1))

    @pl.when(greeted > 0)
    def _():
        pl.semaphore_wait(barrier, greeted)

    for a in range(3):
        if sizes[a] > 1:
            @pl.when(has_lower[a])
            def _():
                signal(ready, **{AXES[a]: me[a] - 1})
    for off in range(2, n):
        @pl.when(ix - off >= 0)
        def _():
            signal(far_ready, gx=ix - off)

    @pl.when(ix == 0)
    def _():
        xh[0] = jnp.zeros(xh.shape[1:], jnp.int32)

    @pl.when(ix == n - 1)
    def _():
        xh[1] = jnp.zeros(xh.shape[1:], jnp.int32)
    for a, halo in ((1, yh), (2, zh)):
        @pl.when(me[a] == 0)
        def _():
            halo[:, 0] = jnp.zeros((n,) + halo.shape[2:], jnp.int32)

        @pl.when(me[a] == sizes[a] - 1)
        def _():
            halo[:, 1] = jnp.zeros((n,) + halo.shape[2:], jnp.int32)

    lane = lax.broadcasted_iota(jnp.int32, (8, lanes), 1)
    line = lax.broadcasted_iota(jnp.int32, (8, lanes), 0)
    row_no = lax.broadcasted_iota(jnp.int32, (rows, lanes), 0)
    lane_no = lax.broadcasted_iota(jnp.int32, (rows, lanes), 1)

    loads[0].wait()
    vol3 = vols[ix]
    vol = vol3.reshape(depth * rows, lanes)
    yedge[0] = vol3[:, 0, :]
    yedge[1] = vol3[:, rows - 1, :]
    first = jnp.zeros((8, lanes), jnp.int32)
    last = jnp.zeros((8, lanes), jnp.int32)
    for v in range(depth * per):
        piece = vol[v * 8:(v + 1) * 8]
        to_last = (2 * v + 1) % lanes
        to_first = (2 * v - 1) % lanes
        last = jnp.where(lane == 2 * v, pltpu.roll(piece, to_last, 1) if to_last else piece, last)
        first = jnp.where(lane == to_first, pltpu.roll(piece, to_first, 1) if to_first else piece, first)
    zedge[0] = first
    zedge[1] = last
    sources = (
        (vols.at[ix, 0], vols.at[ix, depth - 1]),
        (yedge.at[0], yedge.at[1]),
        (zedge.at[0], zedge.at[1]),
    )

    def landing(a, side):
        return xh.at[1 - side] if a == 0 else (None, yh, zh)[a].at[ix, 1 - side]

    def halo_copy(a, side):
        return pltpu.make_async_remote_copy(
            src_ref=sources[a][side], dst_ref=landing(a, side),
            send_sem=halo_send.at[a, side], recv_sem=halo_recv.at[a, 1 - side],
            device_id={AXES[a]: me[a] + (1 if side else -1)}, device_id_type=MESH,
        )

    def edge_to_front(a, side):
        return pltpu.make_async_remote_copy(
            src_ref=sources[a][side], dst_ref=landing(a, side),
            send_sem=front_send.at[2 * a + side], recv_sem=edge_recv.at[ix, 2 * (a - 1) + 1 - side],
            device_id={"gx": 0, AXES[a]: me[a] + (1 if side else -1)}, device_id_type=MESH,
        )

    def raw_to_front():
        return pltpu.make_async_remote_copy(
            src_ref=vols.at[ix], dst_ref=vols.at[ix], send_sem=front_send.at[0], recv_sem=raw_recv.at[ix, 0],
            device_id={"gx": 0}, device_id_type=MESH,
        )

    def last_to_front():
        k = raw_from - 1
        return pltpu.make_async_remote_copy(
            src_ref=vols.at[k, depth - 1], dst_ref=vols.at[k, depth - 1],
            send_sem=front_send.at[0], recv_sem=raw_recv.at[k, 0],
            device_id={"gx": 0}, device_id_type=MESH,
        )

    def frame_to_front():
        return pltpu.make_async_remote_copy(
            src_ref=frames.at[ix], dst_ref=frames.at[ix], send_sem=front_send.at[1], recv_sem=raw_recv.at[ix, 1],
            device_id={"gx": 0}, device_id_type=MESH,
        )

    for a in (2, 1):
        @pl.when(is_raw & has_lower[a])
        def _():
            edge_to_front(a, 0).start()
    for a in (0, 2, 1):
        @pl.when(has_lower[a])
        def _():
            halo_copy(a, 0).start()

    if raw_from > 1:
        @pl.when(ix == raw_from - 1)
        def _():
            last_to_front().start()

    @pl.when(is_raw)
    def _():
        raw_to_front().start()

    loads[2].wait()
    frames[ix] = jnp.where(
        line == 0,
        ((lane >= foot_ref[0, 0, 0, 2]) & (lane < foot_ref[0, 0, 0, 3])).astype(jnp.int32),
        jnp.where(line == 1, foot_ref[0, 0, 0, 0], foot_ref[0, 0, 0, 1]),
    )

    @pl.when(is_raw)
    def _():
        frame_to_front().start()

    above = 0
    for a in range(3):
        above = above + lax.min(sizes[a] - 1 - me[a], 1)

    @pl.when(above > 0)
    def _():
        pl.semaphore_wait(ready, above)

    for a in (0, 2, 1):
        @pl.when(has_upper[a])
        def _():
            halo_copy(a, 1).start()
    for a in (2, 1):
        @pl.when(is_raw & has_upper[a])
        def _():
            edge_to_front(a, 1).start()

    loads[1].wait()

    def inside(b):
        frame = frames[b]
        return (frame[0:1] > 0) & (row_no >= frame[1:2]) & (row_no < frame[2:3])

    def prepare(b):
        ints = vols[b].reshape(depth * rows, lanes)
        d3 = lookup(table_ref[3:4, :], ints, lanes).reshape(depth, rows, lanes)
        dens[pl.ds(b * depth + 1, depth)] = d3
        transmit = jnp.ones((rows, lanes), jnp.float32)
        weights = []
        for x in range(depth):
            sample = 1.0 - jnp.exp(-extent * d3[x])
            weights.append(transmit * sample)
            transmit = transmit * (1.0 - sample)
        alphas[b] = jnp.where(inside(b), 1.0 - transmit, 0.0)
        for c in range(3):
            emit = lookup(table_ref[c:c + 1, :], ints, lanes).reshape(depth, rows, lanes)
            for x in range(depth):
                wemit[b, c, x] = weights[x] * emit[x]
        for x in range(depth):
            d = d3[x]
            up = jnp.where(row_no == 0, 0.0, pltpu.roll(d, 1, 0))
            down = jnp.where(row_no == rows - 1, 0.0, pltpu.roll(d, rows - 1, 0))
            inner[b, 0, x] = 0.5 * (down - up)
            left = jnp.where(lane_no == 0, 0.0, pltpu.roll(d, 1, 1))
            right = jnp.where(lane_no == lanes - 1, 0.0, pltpu.roll(d, lanes - 1, 1))
            inner[b, 1, x] = 0.5 * (right - left)

    half = [
        [jnp.where(has_lower[a], 0.5, 0.0), jnp.where(has_upper[a], 0.5, 0.0)] for a in range(3)
    ]
    even = (lane & 1) == 0
    on_side = (lane == 0) | (lane == lanes - 1)

    def shade(b, span):
        opacity = table_ref[3:4, :]
        half_up = half[1][0] * lookup(opacity, yh[b, 0], lanes)
        half_down = half[1][1] * lookup(opacity, yh[b, 1], lanes)
        sides = jnp.where(even, -half[2][0], half[2][1]) * lookup(opacity, jnp.where(even, zh[b, 0], zh[b, 1]), lanes)
        colour = [[None] * per for _ in range(3)]
        for x in span:
            for h in range(per):
                at = pl.ds(h * 8, 8)
                v = x * per + h
                g_x = 0.5 * (dens[b * depth + x + 2, at, :] - dens[b * depth + x, at, :])
                g_y = inner[b, 0, x, at, :]
                if h == 0:
                    g_y = jnp.where(line == 0, g_y - half_up[x:x + 1, :], g_y)
                if h == per - 1:
                    g_y = jnp.where(line == 7, g_y + half_down[x:x + 1, :], g_y)
                side = pltpu.roll(sides, lanes - 2 * v, 1) if v else sides
                g_z = inner[b, 1, x, at, :]
                g_z = jnp.where(on_side, g_z + side, g_z)
                facing = jnp.abs(g_x * LIGHT[0] + g_y * LIGHT[1] + g_z * LIGHT[2]) * lax.rsqrt(
                    1.0 + (g_x * g_x + g_y * g_y + g_z * g_z)
                )
                lit = 0.35 + 0.65 * facing
                for c in range(3):
                    term = wemit[b, c, x, at, :] * lit
                    colour[c][h] = term if colour[c][h] is None else colour[c][h] + term
        return [jnp.where(inside(b), jnp.concatenate(c, axis=0), 0.0) for c in colour]

    prepare(ix)

    def image_copy(buf, off, s_sem, r_sem):
        return pltpu.make_async_remote_copy(
            src_ref=buf.at[ix], dst_ref=buf.at[ix], send_sem=s_sem.at[off], recv_sem=r_sem.at[off],
            device_id={"gx": lax.rem(ix + off, n)}, device_id_type=MESH,
        )

    def for_images(act):
        for far in range(n - 1, 0, -1):
            @pl.when(ix + far < n)
            def _():
                act(far)

            @pl.when((ix - far >= 1) | ((ix == far) & (far < raw_from)))
            def _():
                act(n - far)

    @pl.when(ix < n - 2)
    def _():
        pl.semaphore_wait(far_ready, n - 2 - ix)
    for_images(lambda off: image_copy(alphas, off, a_send, a_recv).start())

    for a in range(3):
        @pl.when(has_lower[a])
        def _():
            halo_copy(a, 1).wait_recv()

        @pl.when(has_upper[a])
        def _():
            halo_copy(a, 0).wait_recv()
    opacity = table_ref[3:4, :]
    dens[ix * depth] = 2.0 * half[0][0] * lookup(opacity, xh[0], lanes)
    dens[ix * depth + depth + 1] = 2.0 * half[0][1] * lookup(opacity, xh[1], lanes)
    own = shade(ix, range(depth))
    for c in range(3):
        colours[ix, c] = own[c]
    for_images(lambda off: image_copy(colours, off, c_send, c_recv).start())
    loads[3].wait()

    @pl.when(ix == 0)
    def _():
        def step(b, carry):
            for which in range(2):
                pltpu.make_async_remote_copy(
                    src_ref=(vols, frames)[which].at[b], dst_ref=(vols, frames)[which].at[b],
                    send_sem=front_send.at[which], recv_sem=raw_recv.at[b, which],
                    device_id={"gx": 1}, device_id_type=MESH,
                ).wait_recv()
            prepare(b)
            for a, halo in ((1, yh), (2, zh)):
                for side, there in ((0, has_lower[a]), (1, has_upper[a])):
                    @pl.when(there)
                    def _():
                        pltpu.make_async_remote_copy(
                            src_ref=halo.at[b, side], dst_ref=halo.at[b, side],
                            send_sem=front_send.at[0], recv_sem=edge_recv.at[b, 2 * (a - 1) + side],
                            device_id={"gx": 1}, device_id_type=MESH,
                        ).wait_recv()

            @pl.when(b > raw_from)
            def _():
                rest = shade(b - 1, (depth - 1,))
                for c in range(3):
                    colours[b - 1, c] = colours[b - 1, c] + rest[c]
            got = shade(b, range(depth - 1))
            for c in range(3):
                colours[b, c] = got[c]
            return carry

        if raw_from > 1:
            pltpu.make_async_remote_copy(
                src_ref=vols.at[raw_from - 1, depth - 1], dst_ref=vols.at[raw_from - 1, depth - 1],
                send_sem=front_send.at[0], recv_sem=raw_recv.at[raw_from - 1, 0],
                device_id={"gx": 1}, device_id_type=MESH,
            ).wait_recv()
            dens[raw_from * depth] = lookup(opacity, vols[raw_from - 1, depth - 1], lanes)
        lax.fori_loop(raw_from, n, step, 0)
        if n > 1:
            dens[n * depth + 1] = jnp.zeros((rows, lanes), jnp.float32)
            rest = shade(n - 1, (depth - 1,))
            for c in range(3):
                colours[n - 1, c] = colours[n - 1, c] + rest[c]

    for off in range(1, n):
        @pl.when((ix > 0) | (n - off < raw_from))
        def _():
            image_copy(alphas, off, a_send, a_recv).wait_recv()

    clear = [1.0 - alphas[b] for b in range(n)]

    def cover(rank):
        seen = jnp.ones((rows, lanes), jnp.float32)
        for b in range(n):
            seen = seen * jnp.where(rank_ref[b] < rank, clear[b], 1.0)
        return seen

    own_cover = cover(rank_ref[ix])
    alpha = own_cover * alphas[ix]
    total = [own_cover * colours[ix, c] for c in range(3)]
    for off in range(1, n):
        b = lax.rem(ix + off, n)

        @pl.when((ix > 0) | (off < raw_from))
        def _():
            image_copy(colours, n - off, c_send, c_recv).wait_recv()
        seen = cover(rank_ref[b])
        alpha = alpha + seen * alphas[b]
        total = [total[c] + seen * colours[b, c] for c in range(3)]
    for c in range(3):
        out_ref[c] = total[c]
    out_ref[3] = alpha

    for a in range(3):
        @pl.when(has_lower[a])
        def _():
            halo_copy(a, 0).wait_send()

        @pl.when(has_upper[a])
        def _():
            halo_copy(a, 1).wait_send()
    for a in (1, 2):
        for side, there in ((0, has_lower[a]), (1, has_upper[a])):
            @pl.when(is_raw & there)
            def _():
                edge_to_front(a, side).wait_send()

    if raw_from > 1:
        @pl.when(ix == raw_from - 1)
        def _():
            last_to_front().wait_send()

    @pl.when(is_raw)
    def _():
        frame_to_front().wait_send()
        raw_to_front().wait_send()
    for_images(lambda off: image_copy(alphas, off, a_send, a_recv).wait_send())
    for_images(lambda off: image_copy(colours, off, c_send, c_recv).wait_send())


def on_device(sizes, volume, transfer_table, depth_rank, footprint):
    depth, rows, lanes = volume.shape
    n = sizes[0]
    vmem = pl.BlockSpec(memory_space=pltpu.VMEM)
    hbm = pl.BlockSpec(memory_space=pl.ANY)
    return pl.pallas_call(
        functools.partial(kernel, sizes),
        out_shape=pltpu.VMEM((4, rows, lanes), jnp.float32),
        in_specs=[hbm] * 4,
        out_specs=vmem,
        scratch_shapes=[
            pltpu.VMEM((n,) + volume.shape, jnp.int32),
            pltpu.VMEM(transfer_table.shape, jnp.float32),
            pltpu.SMEM(depth_rank.shape, jnp.int32),
            pltpu.SMEM(footprint.shape, jnp.int32),
            pltpu.SemaphoreType.DMA((4,)),
            pltpu.VMEM((n, 8, lanes), jnp.int32),
            pltpu.VMEM((2, depth, lanes), jnp.int32),
            pltpu.VMEM((2, 8, lanes), jnp.int32),
            pltpu.VMEM((2, rows, lanes), jnp.int32),
            pltpu.VMEM((n, 2, depth, lanes), jnp.int32),
            pltpu.VMEM((n, 2, 8, lanes), jnp.int32),
            pltpu.VMEM((n * depth + 2, rows, lanes), jnp.float32),
            pltpu.VMEM((n, 3, depth, rows, lanes), jnp.float32),
            pltpu.VMEM((n, 2, depth, rows, lanes), jnp.float32),
            pltpu.VMEM((n, rows, lanes), jnp.float32),
            pltpu.VMEM((n, 3, rows, lanes), jnp.float32),
            pltpu.SemaphoreType.REGULAR,
            pltpu.SemaphoreType.REGULAR,
            pltpu.SemaphoreType.DMA((3, 2)),
            pltpu.SemaphoreType.DMA((3, 2)),
            pltpu.SemaphoreType.DMA((6,)),
            pltpu.SemaphoreType.DMA((n, 2)),
            pltpu.SemaphoreType.DMA((n, 4)),
            pltpu.SemaphoreType.DMA((n,)),
            pltpu.SemaphoreType.DMA((n,)),
            pltpu.SemaphoreType.DMA((n,)),
            pltpu.SemaphoreType.DMA((n,)),
        ],
        compiler_params=pltpu.CompilerParams(collective_id=0, has_side_effects=True),
        name="raycast",
    )(volume, transfer_table, depth_rank, footprint)


def solution(mesh):
    placed = (P("gx", "gy", "gz"), P(), P(), P("gx", "gy", "gz", None))
    sizes = tuple(mesh.shape[a] for a in AXES)
    return jax.shard_map(
        functools.partial(on_device, sizes), mesh=mesh, in_specs=placed,
        out_specs=P(None, "gy", "gz"), check_vma=False,
    )
```

```python
import functools

import jax
import jax.numpy as jnp
from jax import lax
from jax.experimental import pallas as pl
from jax.experimental.pallas import tpu as pltpu
from jax.sharding import PartitionSpec as P

LIGHT = (1.0 / 3.0, 2.0 / 3.0, 2.0 / 3.0)
AXES = ("gx", "gy", "gz")
MESH = pl.DeviceIdType.MESH


def lookup(table_row, index, lanes):
    entries = table_row.shape[1]
    low = index & (lanes - 1)
    found = None
    for part in range(entries // lanes):
        piece = jnp.broadcast_to(table_row[:, part * lanes:(part + 1) * lanes], index.shape)
        got = jnp.take_along_axis(piece, low, axis=1, mode="promise_in_bounds")
        found = got if found is None else jnp.where(index >= part * lanes, got, found)
    return found


def kernel(sizes, vol_hbm, table_hbm, rank_hbm, foot_hbm, out_ref,
           vols, table_ref, rank_ref, foot_ref, load_sem, frames, yedge, zedge, xh, yh, zh,
           dens, wemit, inner, alphas, colours,
           ready, far_ready, halo_send, halo_recv, front_send, raw_recv, edge_recv, a_send, a_recv, c_send, c_recv):
    n, ny, nz = sizes
    _, depth, rows, lanes = vols.shape
    per = rows // 8
    extent = 4.0 / (depth * n)
    me = [lax.axis_index(a) for a in AXES]
    ix = me[0]

    def first_raw(gy, gz):
        even = 1 - lax.rem(gy + 2, 2)
        return lax.max(1, n - even * (2 - lax.min(gy + gz, 1)))

    raw_from = first_raw(me[1], me[2])
    is_raw = ix >= raw_from

    def wants_edge(a, side):
        step = 1 if side else -1
        gy, gz = me[1] + (step if a == 1 else 0), me[2] + (step if a == 2 else 0)
        return (has_upper if side else has_lower)[a] & (ix >= first_raw(gy, gz))

    has_lower = [me[a] > 0 for a in range(3)]
    has_upper = [me[a] < sizes[a] - 1 for a in range(3)]

    def signal(sem, **where):
        pl.semaphore_signal(sem, inc=1, device_id=where, device_id_type=MESH)

    barrier = pltpu.get_barrier_semaphore()
    for off in range(n - 1, 0, -1):
        @pl.when(ix + off < n)
        def _():
            signal(barrier, gx=ix + off)
    for a in (1, 2):
        if sizes[a] > 1:
            @pl.when(has_upper[a])
            def _():
                signal(barrier, **{AXES[a]: me[a] + 1})

            @pl.when((ix == 0) & has_upper[a])
            def _():
                for k in range(n - 1, 0, -1):
                    signal(barrier, **{"gx": k, AXES[a]: me[a] + 1})

    loads = [
        pltpu.make_async_copy(src, dst, load_sem.at[i])
        for i, (src, dst) in enumerate((
            (vol_hbm, vols.at[ix]), (table_hbm, table_ref), (foot_hbm, foot_ref), (rank_hbm, rank_ref)
        ))
    ]
    for load in loads:
        load.start()

    greeted = ix
    for a in (1, 2):
        greeted = greeted + lax.min(me[a], 1) * (1 + lax.min(ix, 1))

    @pl.when(greeted > 0)
    def _():
        pl.semaphore_wait(barrier, greeted)

    for a in range(3):
        if sizes[a] > 1:
            @pl.when(has_lower[a])
            def _():
                signal(ready, **{AXES[a]: me[a] - 1})
    for off in range(2, n):
        @pl.when(ix - off >= 0)
        def _():
            signal(far_ready, gx=ix - off)

    @pl.when(ix == 0)
    def _():
        xh[0] = jnp.zeros(xh.shape[1:], jnp.int32)

    @pl.when(ix == n - 1)
    def _():
        xh[1] = jnp.zeros(xh.shape[1:], jnp.int32)
    for a, halo in ((1, yh), (2, zh)):
        @pl.when(me[a] == 0)
        def _():
            halo[:, 0] = jnp.zeros((n,) + halo.shape[2:], jnp.int32)

        @pl.when(me[a] == sizes[a] - 1)
        def _():
            halo[:, 1] = jnp.zeros((n,) + halo.shape[2:], jnp.int32)

    lane = lax.broadcasted_iota(jnp.int32, (8, lanes), 1)
    line = lax.broadcasted_iota(jnp.int32, (8, lanes), 0)
    row_no = lax.broadcasted_iota(jnp.int32, (rows, lanes), 0)
    lane_no = lax.broadcasted_iota(jnp.int32, (rows, lanes), 1)

    sources = (
        (vols.at[ix, 0], vols.at[ix, depth - 1]),
        (yedge.at[0], yedge.at[1]),
        (zedge.at[0], zedge.at[1]),
    )

    def landing(a, side):
        return xh.at[1 - side] if a == 0 else (None, yh, zh)[a].at[ix, 1 - side]

    def halo_copy(a, side):
        return pltpu.make_async_remote_copy(
            src_ref=sources[a][side], dst_ref=landing(a, side),
            send_sem=halo_send.at[a, side], recv_sem=halo_recv.at[a, 1 - side],
            device_id={AXES[a]: me[a] + (1 if side else -1)}, device_id_type=MESH,
        )

    def edge_to_front(a, side):
        return pltpu.make_async_remote_copy(
            src_ref=sources[a][side], dst_ref=landing(a, side),
            send_sem=front_send.at[2 * a + side], recv_sem=edge_recv.at[ix, 2 * (a - 1) + 1 - side],
            device_id={"gx": 0, AXES[a]: me[a] + (1 if side else -1)}, device_id_type=MESH,
        )

    def raw_to_front():
        return pltpu.make_async_remote_copy(
            src_ref=vols.at[ix], dst_ref=vols.at[ix], send_sem=front_send.at[0], recv_sem=raw_recv.at[ix, 0],
            device_id={"gx": 0}, device_id_type=MESH,
        )

    def last_to_front():
        k = raw_from - 1
        return pltpu.make_async_remote_copy(
            src_ref=vols.at[k, depth - 1], dst_ref=vols.at[k, depth - 1],
            send_sem=front_send.at[0], recv_sem=raw_recv.at[k, 0],
            device_id={"gx": 0}, device_id_type=MESH,
        )

    def frame_to_front():
        return pltpu.make_async_remote_copy(
            src_ref=frames.at[ix], dst_ref=frames.at[ix], send_sem=front_send.at[1], recv_sem=raw_recv.at[ix, 1],
            device_id={"gx": 0}, device_id_type=MESH,
        )

    loads[0].wait()

    @pl.when(has_lower[0])
    def _():
        halo_copy(0, 0).start()

    def send_raw(when):
        @pl.when(when & (ix > 0) & (ix == raw_from - 1) & (raw_from < n))
        def _():
            last_to_front().start()

        @pl.when(when & is_raw)
        def _():
            raw_to_front().start()

    at_first = me[1] + me[2] == 0
    send_raw(at_first)
    vol3 = vols[ix]
    vol = vol3.reshape(depth * rows, lanes)
    yedge[0] = vol3[:, 0, :]
    yedge[1] = vol3[:, rows - 1, :]

    def send_lower(a):
        @pl.when(wants_edge(a, 0))
        def _():
            edge_to_front(a, 0).start()

        @pl.when(has_lower[a])
        def _():
            halo_copy(a, 0).start()

    send_lower(1)
    first = jnp.zeros((8, lanes), jnp.int32)
    last = jnp.zeros((8, lanes), jnp.int32)
    for v in range(depth * per):
        piece = vol[v * 8:(v + 1) * 8]
        to_last = (2 * v + 1) % lanes
        to_first = (2 * v - 1) % lanes
        last = jnp.where(lane == 2 * v, pltpu.roll(piece, to_last, 1) if to_last else piece, last)
        first = jnp.where(lane == to_first, pltpu.roll(piece, to_first, 1) if to_first else piece, first)
    zedge[0] = first
    zedge[1] = last
    send_lower(2)
    send_raw(jnp.logical_not(at_first))
    loads[2].wait()
    frames[ix] = jnp.where(
        line == 0,
        ((lane >= foot_ref[0, 0, 0, 2]) & (lane < foot_ref[0, 0, 0, 3])).astype(jnp.int32),
        jnp.where(line == 1, foot_ref[0, 0, 0, 0], foot_ref[0, 0, 0, 1]),
    )

    @pl.when(is_raw)
    def _():
        frame_to_front().start()

    above = 0
    for a in range(3):
        above = above + lax.min(sizes[a] - 1 - me[a], 1)

    @pl.when(above > 0)
    def _():
        pl.semaphore_wait(ready, above)

    for a in (0, 2, 1):
        @pl.when(has_upper[a])
        def _():
            halo_copy(a, 1).start()
    for a in (2, 1):
        @pl.when(wants_edge(a, 1))
        def _():
            edge_to_front(a, 1).start()

    loads[1].wait()

    def inside(b):
        frame = frames[b]
        return (frame[0:1] > 0) & (row_no >= frame[1:2]) & (row_no < frame[2:3])

    def prepare(b):
        ints = vols[b].reshape(depth * rows, lanes)
        d3 = lookup(table_ref[3:4, :], ints, lanes).reshape(depth, rows, lanes)
        dens[pl.ds(b * depth + 1, depth)] = d3
        transmit = jnp.ones((rows, lanes), jnp.float32)
        weights = []
        for x in range(depth):
            sample = 1.0 - jnp.exp(-extent * d3[x])
            weights.append(transmit * sample)
            transmit = transmit * (1.0 - sample)
        alphas[b] = jnp.where(inside(b), 1.0 - transmit, 0.0)
        for c in range(3):
            emit = lookup(table_ref[c:c + 1, :], ints, lanes).reshape(depth, rows, lanes)
            for x in range(depth):
                wemit[b, c, x] = weights[x] * emit[x]
        for x in range(depth):
            d = d3[x]
            up = jnp.where(row_no == 0, 0.0, pltpu.roll(d, 1, 0))
            down = jnp.where(row_no == rows - 1, 0.0, pltpu.roll(d, rows - 1, 0))
            inner[b, 0, x] = 0.5 * (down - up)
            left = jnp.where(lane_no == 0, 0.0, pltpu.roll(d, 1, 1))
            right = jnp.where(lane_no == lanes - 1, 0.0, pltpu.roll(d, lanes - 1, 1))
            inner[b, 1, x] = 0.5 * (right - left)

    half = [
        [jnp.where(has_lower[a], 0.5, 0.0), jnp.where(has_upper[a], 0.5, 0.0)] for a in range(3)
    ]
    even = (lane & 1) == 0
    on_side = (lane == 0) | (lane == lanes - 1)

    def shade(b, span):
        opacity = table_ref[3:4, :]
        half_up = half[1][0] * lookup(opacity, yh[b, 0], lanes)
        half_down = half[1][1] * lookup(opacity, yh[b, 1], lanes)
        sides = jnp.where(even, -half[2][0], half[2][1]) * lookup(opacity, jnp.where(even, zh[b, 0], zh[b, 1]), lanes)
        colour = [[None] * per for _ in range(3)]
        for x in span:
            for h in range(per):
                at = pl.ds(h * 8, 8)
                v = x * per + h
                g_x = 0.5 * (dens[b * depth + x + 2, at, :] - dens[b * depth + x, at, :])
                g_y = inner[b, 0, x, at, :]
                if h == 0:
                    g_y = jnp.where(line == 0, g_y - half_up[x:x + 1, :], g_y)
                if h == per - 1:
                    g_y = jnp.where(line == 7, g_y + half_down[x:x + 1, :], g_y)
                side = pltpu.roll(sides, lanes - 2 * v, 1) if v else sides
                g_z = inner[b, 1, x, at, :]
                g_z = jnp.where(on_side, g_z + side, g_z)
                facing = jnp.abs(g_x * LIGHT[0] + g_y * LIGHT[1] + g_z * LIGHT[2]) * lax.rsqrt(
                    1.0 + (g_x * g_x + g_y * g_y + g_z * g_z)
                )
                lit = 0.35 + 0.65 * facing
                for c in range(3):
                    term = wemit[b, c, x, at, :] * lit
                    colour[c][h] = term if colour[c][h] is None else colour[c][h] + term
        return [jnp.where(inside(b), jnp.concatenate(c, axis=0), 0.0) for c in colour]

    prepare(ix)

    def image_copy(buf, off, s_sem, r_sem):
        return pltpu.make_async_remote_copy(
            src_ref=buf.at[ix], dst_ref=buf.at[ix], send_sem=s_sem.at[off], recv_sem=r_sem.at[off],
            device_id={"gx": lax.rem(ix + off, n)}, device_id_type=MESH,
        )

    def for_images(act):
        for far in range(n - 1, 0, -1):
            @pl.when(ix + far < n)
            def _():
                act(far)

            @pl.when((ix - far >= 1) | ((ix == far) & (far < raw_from)))
            def _():
                act(n - far)

    @pl.when(ix < n - 2)
    def _():
        pl.semaphore_wait(far_ready, n - 2 - ix)
    for_images(lambda off: image_copy(alphas, off, a_send, a_recv).start())

    for a in range(3):
        @pl.when(has_lower[a])
        def _():
            halo_copy(a, 1).wait_recv()

        @pl.when(has_upper[a])
        def _():
            halo_copy(a, 0).wait_recv()
    opacity = table_ref[3:4, :]
    dens[ix * depth] = 2.0 * half[0][0] * lookup(opacity, xh[0], lanes)
    dens[ix * depth + depth + 1] = 2.0 * half[0][1] * lookup(opacity, xh[1], lanes)
    own = shade(ix, range(depth))
    for c in range(3):
        colours[ix, c] = own[c]
    for_images(lambda off: image_copy(colours, off, c_send, c_recv).start())
    loads[3].wait()

    @pl.when((ix == 0) & (raw_from < n))
    def _():
        def step(b, carry):
            for which in range(2):
                pltpu.make_async_remote_copy(
                    src_ref=(vols, frames)[which].at[b], dst_ref=(vols, frames)[which].at[b],
                    send_sem=front_send.at[which], recv_sem=raw_recv.at[b, which],
                    device_id={"gx": 1}, device_id_type=MESH,
                ).wait_recv()
            prepare(b)
            for a, halo in ((1, yh), (2, zh)):
                for side, there in ((0, has_lower[a]), (1, has_upper[a])):
                    @pl.when(there)
                    def _():
                        pltpu.make_async_remote_copy(
                            src_ref=halo.at[b, side], dst_ref=halo.at[b, side],
                            send_sem=front_send.at[0], recv_sem=edge_recv.at[b, 2 * (a - 1) + side],
                            device_id={"gx": 1}, device_id_type=MESH,
                        ).wait_recv()

            @pl.when(b > raw_from)
            def _():
                rest = shade(b - 1, (depth - 1,))
                for c in range(3):
                    colours[b - 1, c] = colours[b - 1, c] + rest[c]
            got = shade(b, range(depth - 1))
            for c in range(3):
                colours[b, c] = got[c]
            return carry

        @pl.when(raw_from > 1)
        def _():
            pltpu.make_async_remote_copy(
                src_ref=vols.at[raw_from - 1, depth - 1], dst_ref=vols.at[raw_from - 1, depth - 1],
                send_sem=front_send.at[0], recv_sem=raw_recv.at[raw_from - 1, 0],
                device_id={"gx": 1}, device_id_type=MESH,
            ).wait_recv()
            dens[raw_from * depth] = lookup(opacity, vols[raw_from - 1, depth - 1], lanes)
        lax.fori_loop(raw_from, n, step, 0)
        dens[n * depth + 1] = jnp.zeros((rows, lanes), jnp.float32)
        rest = shade(n - 1, (depth - 1,))
        for c in range(3):
            colours[n - 1, c] = colours[n - 1, c] + rest[c]

    for off in range(1, n):
        @pl.when((ix > 0) | (n - off < raw_from))
        def _():
            image_copy(alphas, off, a_send, a_recv).wait_recv()

    clear = [1.0 - alphas[b] for b in range(n)]

    def cover(rank):
        seen = jnp.ones((rows, lanes), jnp.float32)
        for b in range(n):
            seen = seen * jnp.where(rank_ref[b] < rank, clear[b], 1.0)
        return seen

    order = [lax.rem(ix + off, n) for off in range(n)]
    covers = [cover(rank_ref[b]) for b in order]
    alpha = covers[0] * alphas[ix]
    for off in range(1, n):
        alpha = alpha + covers[off] * alphas[order[off]]
    out_ref[3] = alpha
    total = [covers[0] * colours[ix, c] for c in range(3)]
    for off in range(1, n):
        @pl.when((ix > 0) | (off < raw_from))
        def _():
            image_copy(colours, n - off, c_send, c_recv).wait_recv()
        total = [total[c] + covers[off] * colours[order[off], c] for c in range(3)]
    for c in range(3):
        out_ref[c] = total[c]

    for a in range(3):
        @pl.when(has_lower[a])
        def _():
            halo_copy(a, 0).wait_send()

        @pl.when(has_upper[a])
        def _():
            halo_copy(a, 1).wait_send()
    for a in (1, 2):
        for side in range(2):
            @pl.when(wants_edge(a, side))
            def _():
                edge_to_front(a, side).wait_send()

    @pl.when((ix > 0) & (ix == raw_from - 1) & (raw_from < n))
    def _():
        last_to_front().wait_send()

    @pl.when(is_raw)
    def _():
        frame_to_front().wait_send()
        raw_to_front().wait_send()
    for_images(lambda off: image_copy(alphas, off, a_send, a_recv).wait_send())
    for_images(lambda off: image_copy(colours, off, c_send, c_recv).wait_send())


def on_device(sizes, volume, transfer_table, depth_rank, footprint):
    depth, rows, lanes = volume.shape
    n = sizes[0]
    vmem = pl.BlockSpec(memory_space=pltpu.VMEM)
    hbm = pl.BlockSpec(memory_space=pl.ANY)
    return pl.pallas_call(
        functools.partial(kernel, sizes),
        out_shape=pltpu.VMEM((4, rows, lanes), jnp.float32),
        in_specs=[hbm] * 4,
        out_specs=vmem,
        scratch_shapes=[
            pltpu.VMEM((n,) + volume.shape, jnp.int32),
            pltpu.VMEM(transfer_table.shape, jnp.float32),
            pltpu.SMEM(depth_rank.shape, jnp.int32),
            pltpu.SMEM(footprint.shape, jnp.int32),
            pltpu.SemaphoreType.DMA((4,)),
            pltpu.VMEM((n, 8, lanes), jnp.int32),
            pltpu.VMEM((2, depth, lanes), jnp.int32),
            pltpu.VMEM((2, 8, lanes), jnp.int32),
            pltpu.VMEM((2, rows, lanes), jnp.int32),
            pltpu.VMEM((n, 2, depth, lanes), jnp.int32),
            pltpu.VMEM((n, 2, 8, lanes), jnp.int32),
            pltpu.VMEM((n * depth + 2, rows, lanes), jnp.float32),
            pltpu.VMEM((n, 3, depth, rows, lanes), jnp.float32),
            pltpu.VMEM((n, 2, depth, rows, lanes), jnp.float32),
            pltpu.VMEM((n, rows, lanes), jnp.float32),
            pltpu.VMEM((n, 3, rows, lanes), jnp.float32),
            pltpu.SemaphoreType.REGULAR,
            pltpu.SemaphoreType.REGULAR,
            pltpu.SemaphoreType.DMA((3, 2)),
            pltpu.SemaphoreType.DMA((3, 2)),
            pltpu.SemaphoreType.DMA((6,)),
            pltpu.SemaphoreType.DMA((n, 2)),
            pltpu.SemaphoreType.DMA((n, 4)),
            pltpu.SemaphoreType.DMA((n,)),
            pltpu.SemaphoreType.DMA((n,)),
            pltpu.SemaphoreType.DMA((n,)),
            pltpu.SemaphoreType.DMA((n,)),
        ],
        compiler_params=pltpu.CompilerParams(collective_id=0, has_side_effects=True),
        name="raycast",
    )(volume, transfer_table, depth_rank, footprint)


def solution(mesh):
    placed = (P("gx", "gy", "gz"), P(), P(), P("gx", "gy", "gz", None))
    sizes = tuple(mesh.shape[a] for a in AXES)
    return jax.shard_map(
        functools.partial(on_device, sizes), mesh=mesh, in_specs=placed,
        out_specs=P(None, "gy", "gz"), check_vma=False,
    )
```

```python
import functools

import jax
import jax.numpy as jnp
from jax import lax
from jax.experimental import pallas as pl
from jax.experimental.pallas import tpu as pltpu
from jax.sharding import PartitionSpec as P

LIGHT = (1.0 / 3.0, 2.0 / 3.0, 2.0 / 3.0)
AXES = ("gx", "gy", "gz")
MESH = pl.DeviceIdType.MESH


def lookup(table, index, lanes):
    count, entries = table.shape
    low = index & (lanes - 1)
    found = [None] * count
    for part in range(entries // lanes):
        for t in range(count):
            piece = jnp.broadcast_to(table[t:t + 1, part * lanes:(part + 1) * lanes], index.shape)
            got = jnp.take_along_axis(piece, low, axis=1, mode="promise_in_bounds")
            found[t] = got if part == 0 else jnp.where(index >= part * lanes, got, found[t])
    return found


def kernel(sizes, vol_hbm, table_hbm, rank_hbm, foot_hbm, out_ref,
           vols, table_ref, rank_ref, foot_ref, load_sem, frames, zedge, xh, yh, zh,
           dens, wemit, inner, alphas, colours,
           ready, far_ready, halo_send, halo_recv, front_send, raw_recv, edge_recv, a_send, a_recv, c_send, c_recv):
    n, ny, nz = sizes
    _, depth, rows, lanes = vols.shape
    per = rows // 8
    extent = 4.0 / (depth * n)
    me = [lax.axis_index(a) for a in AXES]
    ix = me[0]

    def first_raw(gy, gz):
        even = 1 - lax.rem(gy + 2, 2)
        return lax.max(1, n - even * (3 - 2 * lax.min(gy + gz, 1)))

    raw_from = first_raw(me[1], me[2])
    is_raw = ix >= raw_from

    def wants_edge(a, side):
        step = 1 if side else -1
        gy, gz = me[1] + (step if a == 1 else 0), me[2] + (step if a == 2 else 0)
        return (has_upper if side else has_lower)[a] & (ix >= first_raw(gy, gz))

    has_lower = [me[a] > 0 for a in range(3)]
    has_upper = [me[a] < sizes[a] - 1 for a in range(3)]

    def signal(sem, **where):
        pl.semaphore_signal(sem, inc=1, device_id=where, device_id_type=MESH)

    loads = [
        pltpu.make_async_copy(src, dst, load_sem.at[i])
        for i, (src, dst) in enumerate((
            (vol_hbm, vols.at[ix]), (table_hbm, table_ref), (foot_hbm, foot_ref), (rank_hbm, rank_ref)
        ))
    ]
    for load in loads:
        load.start()

    barrier = pltpu.get_barrier_semaphore()
    for off in range(n - 1, 0, -1):
        @pl.when(ix + off < n)
        def _():
            signal(barrier, gx=ix + off)
    for a in (1, 2):
        if sizes[a] > 1:
            @pl.when(has_upper[a])
            def _():
                signal(barrier, **{AXES[a]: me[a] + 1})

            @pl.when((ix == 0) & has_upper[a])
            def _():
                for k in range(n - 1, 0, -1):
                    signal(barrier, **{"gx": k, AXES[a]: me[a] + 1})

    greeted = ix
    for a in (1, 2):
        greeted = greeted + lax.min(me[a], 1) * (1 + lax.min(ix, 1))

    @pl.when(greeted > 0)
    def _():
        pl.semaphore_wait(barrier, greeted)

    for a in range(3):
        if sizes[a] > 1:
            @pl.when(has_lower[a])
            def _():
                signal(ready.at[a], **{AXES[a]: me[a] - 1})
    for off in range(2, n):
        @pl.when(ix - off >= 0)
        def _():
            signal(far_ready, gx=ix - off)

    @pl.when(ix == 0)
    def _():
        xh[0] = jnp.zeros(xh.shape[1:], jnp.int32)

    @pl.when(ix == n - 1)
    def _():
        xh[1] = jnp.zeros(xh.shape[1:], jnp.int32)
    for a, halo in ((1, yh), (2, zh)):
        @pl.when(me[a] == 0)
        def _():
            halo[:, 0] = jnp.zeros((n,) + halo.shape[2:], jnp.int32)

        @pl.when(me[a] == sizes[a] - 1)
        def _():
            halo[:, 1] = jnp.zeros((n,) + halo.shape[2:], jnp.int32)

    lane = lax.broadcasted_iota(jnp.int32, (8, lanes), 1)
    line = lax.broadcasted_iota(jnp.int32, (8, lanes), 0)
    row_no = lax.broadcasted_iota(jnp.int32, (rows, lanes), 0)
    lane_no = lax.broadcasted_iota(jnp.int32, (rows, lanes), 1)

    sources = (
        (vols.at[ix, 0], vols.at[ix, depth - 1]),
        (vols.at[ix, :, 0], vols.at[ix, :, rows - 1]),
        (zedge.at[0], zedge.at[1]),
    )

    def landing(a, side):
        return xh.at[1 - side] if a == 0 else (None, yh, zh)[a].at[ix, 1 - side]

    def halo_copy(a, side):
        return pltpu.make_async_remote_copy(
            src_ref=sources[a][side], dst_ref=landing(a, side),
            send_sem=halo_send.at[a, side], recv_sem=halo_recv.at[a, 1 - side],
            device_id={AXES[a]: me[a] + (1 if side else -1)}, device_id_type=MESH,
        )

    def edge_to_front(a, side):
        return pltpu.make_async_remote_copy(
            src_ref=sources[a][side], dst_ref=landing(a, side),
            send_sem=front_send.at[2 * a + side], recv_sem=edge_recv.at[ix, 2 * (a - 1) + 1 - side],
            device_id={"gx": 0, AXES[a]: me[a] + (1 if side else -1)}, device_id_type=MESH,
        )

    def raw_to_front():
        return pltpu.make_async_remote_copy(
            src_ref=vols.at[ix], dst_ref=vols.at[ix], send_sem=front_send.at[0], recv_sem=raw_recv.at[ix, 0],
            device_id={"gx": 0}, device_id_type=MESH,
        )

    def last_to_front():
        k = raw_from - 1
        return pltpu.make_async_remote_copy(
            src_ref=vols.at[k, depth - 1], dst_ref=vols.at[k, depth - 1],
            send_sem=front_send.at[0], recv_sem=raw_recv.at[k, 0],
            device_id={"gx": 0}, device_id_type=MESH,
        )

    def frame_to_front():
        return pltpu.make_async_remote_copy(
            src_ref=frames.at[ix], dst_ref=frames.at[ix], send_sem=front_send.at[1], recv_sem=raw_recv.at[ix, 1],
            device_id={"gx": 0}, device_id_type=MESH,
        )

    loads[0].wait()

    @pl.when(has_lower[0])
    def _():
        halo_copy(0, 0).start()

    def send_raw(when):
        @pl.when(when & (ix > 0) & (ix == raw_from - 1) & (raw_from < n))
        def _():
            last_to_front().start()

        @pl.when(when & is_raw)
        def _():
            raw_to_front().start()

    at_first = me[1] + me[2] == 0
    send_raw(at_first)
    vol3 = vols[ix]
    vol = vol3.reshape(depth * rows, lanes)

    def send_lower(a):
        @pl.when(wants_edge(a, 0))
        def _():
            edge_to_front(a, 0).start()

        @pl.when(has_lower[a])
        def _():
            halo_copy(a, 0).start()

    send_lower(1)
    first = jnp.zeros((8, lanes), jnp.int32)
    last = jnp.zeros((8, lanes), jnp.int32)
    for v in range(depth * per):
        piece = vol[v * 8:(v + 1) * 8]
        to_last = (2 * v + 1) % lanes
        to_first = (2 * v - 1) % lanes
        last = jnp.where(lane == 2 * v, pltpu.roll(piece, to_last, 1) if to_last else piece, last)
        first = jnp.where(lane == to_first, pltpu.roll(piece, to_first, 1) if to_first else piece, first)
    zedge[0] = first
    zedge[1] = last
    send_lower(2)
    send_raw(jnp.logical_not(at_first))
    loads[2].wait()
    frames[ix] = jnp.where(
        line == 0,
        ((lane >= foot_ref[0, 0, 0, 2]) & (lane < foot_ref[0, 0, 0, 3])).astype(jnp.int32),
        jnp.where(line == 1, foot_ref[0, 0, 0, 0], foot_ref[0, 0, 0, 1]),
    )

    @pl.when(is_raw)
    def _():
        frame_to_front().start()

    for a in (0, 1, 2):
        @pl.when(has_upper[a])
        def _():
            pl.semaphore_wait(ready.at[a], 1)
            halo_copy(a, 1).start()
    for a in (2, 1):
        @pl.when(wants_edge(a, 1))
        def _():
            edge_to_front(a, 1).start()

    loads[1].wait()

    def inside(b):
        frame = frames[b]
        return (frame[0:1] > 0) & (row_no >= frame[1:2]) & (row_no < frame[2:3])

    def prepare(b):
        transmit = jnp.ones((rows, lanes), jnp.float32)
        d3 = []
        for x in range(depth):
            found = lookup(table_ref, vols[b, x], lanes)
            d3.append(found[3])
            dens[b * depth + x + 1] = d3[x]
            sample = 1.0 - jnp.exp(-extent * d3[x])
            weight = transmit * sample
            transmit = transmit * (1.0 - sample)
            for c in range(3):
                wemit[b, c, x] = weight * found[c]
        alphas[b] = jnp.where(inside(b), 1.0 - transmit, 0.0)
        for x in range(depth):
            d = d3[x]
            up = jnp.where(row_no == 0, 0.0, pltpu.roll(d, 1, 0))
            down = jnp.where(row_no == rows - 1, 0.0, pltpu.roll(d, rows - 1, 0))
            inner[b, 0, x] = 0.5 * (down - up)
            left = jnp.where(lane_no == 0, 0.0, pltpu.roll(d, 1, 1))
            right = jnp.where(lane_no == lanes - 1, 0.0, pltpu.roll(d, lanes - 1, 1))
            inner[b, 1, x] = 0.5 * (right - left)

    half = [
        [jnp.where(has_lower[a], 0.5, 0.0), jnp.where(has_upper[a], 0.5, 0.0)] for a in range(3)
    ]
    even = (lane & 1) == 0
    on_side = (lane == 0) | (lane == lanes - 1)

    def shade(b, span):
        opacity = table_ref[3:4, :]
        half_up = half[1][0] * lookup(opacity, yh[b, 0], lanes)[0]
        half_down = half[1][1] * lookup(opacity, yh[b, 1], lanes)[0]
        sides = jnp.where(even, -half[2][0], half[2][1]) * lookup(opacity, jnp.where(even, zh[b, 0], zh[b, 1]), lanes)[0]
        colour = [[None] * per for _ in range(3)]
        for x in span:
            for h in range(per):
                at = pl.ds(h * 8, 8)
                v = x * per + h
                g_x = 0.5 * (dens[b * depth + x + 2, at, :] - dens[b * depth + x, at, :])
                g_y = inner[b, 0, x, at, :]
                if h == 0:
                    g_y = jnp.where(line == 0, g_y - half_up[x:x + 1, :], g_y)
                if h == per - 1:
                    g_y = jnp.where(line == 7, g_y + half_down[x:x + 1, :], g_y)
                side = pltpu.roll(sides, lanes - 2 * v, 1) if v else sides
                g_z = inner[b, 1, x, at, :]
                g_z = jnp.where(on_side, g_z + side, g_z)
                facing = jnp.abs(g_x * LIGHT[0] + g_y * LIGHT[1] + g_z * LIGHT[2]) * lax.rsqrt(
                    1.0 + (g_x * g_x + g_y * g_y + g_z * g_z)
                )
                lit = 0.35 + 0.65 * facing
                for c in range(3):
                    term = wemit[b, c, x, at, :] * lit
                    colour[c][h] = term if colour[c][h] is None else colour[c][h] + term
        return [jnp.where(inside(b), jnp.concatenate(c, axis=0), 0.0) for c in colour]

    prepare(ix)

    def image_copy(buf, off, s_sem, r_sem):
        return pltpu.make_async_remote_copy(
            src_ref=buf.at[ix], dst_ref=buf.at[ix], send_sem=s_sem.at[off], recv_sem=r_sem.at[off],
            device_id={"gx": lax.rem(ix + off, n)}, device_id_type=MESH,
        )

    def for_images(act):
        for far in range(n - 1, 0, -1):
            @pl.when(ix + far < n)
            def _():
                act(far)

            @pl.when((ix - far >= 1) | ((ix == far) & (far < raw_from)))
            def _():
                act(n - far)

    @pl.when(ix < n - 2)
    def _():
        pl.semaphore_wait(far_ready, n - 2 - ix)
    for_images(lambda off: image_copy(alphas, off, a_send, a_recv).start())

    for a in range(3):
        @pl.when(has_lower[a])
        def _():
            halo_copy(a, 1).wait_recv()

        @pl.when(has_upper[a])
        def _():
            halo_copy(a, 0).wait_recv()
    opacity = table_ref[3:4, :]
    dens[ix * depth] = 2.0 * half[0][0] * lookup(opacity, xh[0], lanes)[0]
    dens[ix * depth + depth + 1] = 2.0 * half[0][1] * lookup(opacity, xh[1], lanes)[0]
    own = shade(ix, range(depth))
    for c in range(3):
        colours[ix, c] = own[c]
    for_images(lambda off: image_copy(colours, off, c_send, c_recv).start())
    loads[3].wait()

    @pl.when((ix == 0) & (raw_from < n))
    def _():
        def step(b, carry):
            for which in range(2):
                pltpu.make_async_remote_copy(
                    src_ref=(vols, frames)[which].at[b], dst_ref=(vols, frames)[which].at[b],
                    send_sem=front_send.at[which], recv_sem=raw_recv.at[b, which],
                    device_id={"gx": 1}, device_id_type=MESH,
                ).wait_recv()
            prepare(b)
            for a, halo in ((1, yh), (2, zh)):
                for side, there in ((0, has_lower[a]), (1, has_upper[a])):
                    @pl.when(there)
                    def _():
                        pltpu.make_async_remote_copy(
                            src_ref=halo.at[b, side], dst_ref=halo.at[b, side],
                            send_sem=front_send.at[0], recv_sem=edge_recv.at[b, 2 * (a - 1) + side],
                            device_id={"gx": 1}, device_id_type=MESH,
                        ).wait_recv()

            def cast(span, follows):
                got = shade(b, span)
                rest = shade(b - 1, (depth - 1,)) if follows else None
                for c in range(3):
                    colours[b, c] = got[c]
                    if follows:
                        colours[b - 1, c] = colours[b - 1, c] + rest[c]

            for is_last, span in ((False, range(depth - 1)), (True, range(depth))):
                for follows in (False, True):
                    @pl.when(((b == n - 1) == is_last) & ((b > raw_from) == follows))
                    def _():
                        cast(span, follows)
            return carry

        dens[n * depth + 1] = jnp.zeros((rows, lanes), jnp.float32)

        @pl.when(raw_from > 1)
        def _():
            pltpu.make_async_remote_copy(
                src_ref=vols.at[raw_from - 1, depth - 1], dst_ref=vols.at[raw_from - 1, depth - 1],
                send_sem=front_send.at[0], recv_sem=raw_recv.at[raw_from - 1, 0],
                device_id={"gx": 1}, device_id_type=MESH,
            ).wait_recv()
            dens[raw_from * depth] = lookup(opacity, vols[raw_from - 1, depth - 1], lanes)[0]
        lax.fori_loop(raw_from, n, step, 0)

    for off in range(1, n):
        @pl.when((ix > 0) | (n - off < raw_from))
        def _():
            image_copy(alphas, off, a_send, a_recv).wait_recv()

    clear = [1.0 - alphas[b] for b in range(n)]

    def cover(rank):
        seen = jnp.ones((rows, lanes), jnp.float32)
        for b in range(n):
            seen = seen * jnp.where(rank_ref[b] < rank, clear[b], 1.0)
        return seen

    order = [lax.rem(ix + off, n) for off in range(n)]
    covers = [cover(rank_ref[b]) for b in order]
    alpha = covers[0] * alphas[ix]
    for off in range(1, n):
        alpha = alpha + covers[off] * alphas[order[off]]
    out_ref[3] = alpha
    for a in range(3):
        @pl.when(has_lower[a])
        def _():
            halo_copy(a, 0).wait_send()

        @pl.when(has_upper[a])
        def _():
            halo_copy(a, 1).wait_send()
    for a in (1, 2):
        for side in range(2):
            @pl.when(wants_edge(a, side))
            def _():
                edge_to_front(a, side).wait_send()

    @pl.when((ix > 0) & (ix == raw_from - 1) & (raw_from < n))
    def _():
        last_to_front().wait_send()

    @pl.when(is_raw)
    def _():
        frame_to_front().wait_send()
        raw_to_front().wait_send()
    for_images(lambda off: image_copy(alphas, off, a_send, a_recv).wait_send())
    for_images(lambda off: image_copy(colours, off, c_send, c_recv).wait_send())

    total = [covers[0] * colours[ix, c] for c in range(3)]
    for off in range(1, n):
        @pl.when((ix > 0) | (off < raw_from))
        def _():
            image_copy(colours, n - off, c_send, c_recv).wait_recv()
        total = [total[c] + covers[off] * colours[order[off], c] for c in range(3)]
    for c in range(3):
        out_ref[c] = total[c]


def on_device(sizes, volume, transfer_table, depth_rank, footprint):
    depth, rows, lanes = volume.shape
    n = sizes[0]
    vmem = pl.BlockSpec(memory_space=pltpu.VMEM)
    hbm = pl.BlockSpec(memory_space=pl.ANY)
    return pl.pallas_call(
        functools.partial(kernel, sizes),
        out_shape=pltpu.VMEM((4, rows, lanes), jnp.float32),
        in_specs=[hbm] * 4,
        out_specs=vmem,
        scratch_shapes=[
            pltpu.VMEM((n,) + volume.shape, jnp.int32),
            pltpu.VMEM(transfer_table.shape, jnp.float32),
            pltpu.SMEM(depth_rank.shape, jnp.int32),
            pltpu.SMEM(footprint.shape, jnp.int32),
            pltpu.SemaphoreType.DMA((4,)),
            pltpu.VMEM((n, 8, lanes), jnp.int32),
            pltpu.VMEM((2, 8, lanes), jnp.int32),
            pltpu.VMEM((2, rows, lanes), jnp.int32),
            pltpu.VMEM((n, 2, depth, lanes), jnp.int32),
            pltpu.VMEM((n, 2, 8, lanes), jnp.int32),
            pltpu.VMEM((n * depth + 2, rows, lanes), jnp.float32),
            pltpu.VMEM((n, 3, depth, rows, lanes), jnp.float32),
            pltpu.VMEM((n, 2, depth, rows, lanes), jnp.float32),
            pltpu.VMEM((n, rows, lanes), jnp.float32),
            pltpu.VMEM((n, 3, rows, lanes), jnp.float32),
            pltpu.SemaphoreType.REGULAR((3,)),
            pltpu.SemaphoreType.REGULAR,
            pltpu.SemaphoreType.DMA((3, 2)),
            pltpu.SemaphoreType.DMA((3, 2)),
            pltpu.SemaphoreType.DMA((6,)),
            pltpu.SemaphoreType.DMA((n, 2)),
            pltpu.SemaphoreType.DMA((n, 4)),
            pltpu.SemaphoreType.DMA((n,)),
            pltpu.SemaphoreType.DMA((n,)),
            pltpu.SemaphoreType.DMA((n,)),
            pltpu.SemaphoreType.DMA((n,)),
        ],
        compiler_params=pltpu.CompilerParams(collective_id=0, has_side_effects=True),
        name="raycast",
    )(volume, transfer_table, depth_rank, footprint)


def solution(mesh):
    placed = (P("gx", "gy", "gz"), P(), P(), P("gx", "gy", "gz", None))
    sizes = tuple(mesh.shape[a] for a in AXES)
    return jax.shard_map(
        functools.partial(on_device, sizes), mesh=mesh, in_specs=placed,
        out_specs=P(None, "gy", "gz"), check_vma=False,
    )
```

```python
import functools

import jax
import jax.numpy as jnp
from jax import lax
from jax.experimental import pallas as pl
from jax.experimental.pallas import tpu as pltpu
from jax.sharding import PartitionSpec as P

LIGHT = (1.0 / 3.0, 2.0 / 3.0, 2.0 / 3.0)
AXES = ("gx", "gy", "gz")
MESH = pl.DeviceIdType.MESH


def lookup(table, index, lanes):
    count, entries = table.shape
    low = index & (lanes - 1)
    found = [None] * count
    for part in range(entries // lanes):
        for t in range(count):
            piece = jnp.broadcast_to(table[t:t + 1, part * lanes:(part + 1) * lanes], index.shape)
            got = jnp.take_along_axis(piece, low, axis=1, mode="promise_in_bounds")
            found[t] = got if part == 0 else jnp.where(index >= part * lanes, got, found[t])
    return found


def kernel(sizes, vol_hbm, table_hbm, rank_hbm, foot_hbm, out_ref,
           vols, table_ref, rank_ref, foot_ref, load_sem, frames, zedge, xh, yh, zh,
           dens, wemit, inner, alphas, colours,
           ready, far_ready, halo_send, halo_recv, front_send, raw_recv, edge_recv, a_send, a_recv, c_send, c_recv):
    n, ny, nz = sizes
    _, depth, rows, lanes = vols.shape
    per = rows // 8
    extent = 4.0 / (depth * n)
    me = [lax.axis_index(a) for a in AXES]
    ix = me[0]

    def first_raw(gy, gz):
        even = 1 - lax.rem(gy + 2, 2)
        return lax.max(1, n - even * (3 - 2 * lax.min(gy + gz, 1)))

    raw_from = first_raw(me[1], me[2])
    is_raw = ix >= raw_from

    def wants_edge(a, side):
        step = 1 if side else -1
        gy, gz = me[1] + (step if a == 1 else 0), me[2] + (step if a == 2 else 0)
        return (has_upper if side else has_lower)[a] & (ix >= first_raw(gy, gz))

    has_lower = [me[a] > 0 for a in range(3)]
    has_upper = [me[a] < sizes[a] - 1 for a in range(3)]

    def signal(sem, **where):
        pl.semaphore_signal(sem, inc=1, device_id=where, device_id_type=MESH)

    cut = max(1, depth // 2)
    head, rest = pl.ds(0, cut), pl.ds(cut, depth - cut)
    loads = [
        pltpu.make_async_copy(src, dst, load_sem.at[i])
        for i, (src, dst) in enumerate((
            (vol_hbm.at[head], vols.at[ix, head]), (table_hbm, table_ref), (foot_hbm, foot_ref), (rank_hbm, rank_ref),
            (vol_hbm.at[rest], vols.at[ix, rest]),
        ))
    ]
    loads = loads if depth > cut else loads[:4]
    for load in (loads[0], *loads[4:], *loads[1:4]):
        load.start()

    barrier = pltpu.get_barrier_semaphore()
    for off in range(n - 1, 0, -1):
        @pl.when(ix + off < n)
        def _():
            signal(barrier, gx=ix + off)
    for a in (1, 2):
        if sizes[a] > 1:
            @pl.when(has_upper[a])
            def _():
                signal(barrier, **{AXES[a]: me[a] + 1})

            @pl.when((ix == 0) & has_upper[a])
            def _():
                for k in range(n - 1, 0, -1):
                    signal(barrier, **{"gx": k, AXES[a]: me[a] + 1})

    greeted = ix
    for a in (1, 2):
        greeted = greeted + lax.min(me[a], 1) * (1 + lax.min(ix, 1))

    @pl.when(greeted > 0)
    def _():
        pl.semaphore_wait(barrier, greeted)

    for a in range(3):
        if sizes[a] > 1:
            @pl.when(has_lower[a])
            def _():
                signal(ready.at[a], **{AXES[a]: me[a] - 1})
    for off in range(2, n):
        @pl.when(ix - off >= 0)
        def _():
            signal(far_ready, gx=ix - off)

    @pl.when(ix == 0)
    def _():
        xh[0] = jnp.zeros(xh.shape[1:], jnp.int32)

    @pl.when(ix == n - 1)
    def _():
        xh[1] = jnp.zeros(xh.shape[1:], jnp.int32)
    for a, halo in ((1, yh), (2, zh)):
        @pl.when(me[a] == 0)
        def _():
            halo[:, 0] = jnp.zeros((n,) + halo.shape[2:], jnp.int32)

        @pl.when(me[a] == sizes[a] - 1)
        def _():
            halo[:, 1] = jnp.zeros((n,) + halo.shape[2:], jnp.int32)

    lane = lax.broadcasted_iota(jnp.int32, (8, lanes), 1)
    line = lax.broadcasted_iota(jnp.int32, (8, lanes), 0)
    row_no = lax.broadcasted_iota(jnp.int32, (rows, lanes), 0)
    lane_no = lax.broadcasted_iota(jnp.int32, (rows, lanes), 1)

    sources = (
        (vols.at[ix, 0], vols.at[ix, depth - 1]),
        (vols.at[ix, :, 0], vols.at[ix, :, rows - 1]),
        (zedge.at[0], zedge.at[1]),
    )

    def landing(a, side):
        return xh.at[1 - side] if a == 0 else (None, yh, zh)[a].at[ix, 1 - side]

    def halo_copy(a, side):
        return pltpu.make_async_remote_copy(
            src_ref=sources[a][side], dst_ref=landing(a, side),
            send_sem=halo_send.at[a, side], recv_sem=halo_recv.at[a, 1 - side],
            device_id={AXES[a]: me[a] + (1 if side else -1)}, device_id_type=MESH,
        )

    def edge_to_front(a, side):
        return pltpu.make_async_remote_copy(
            src_ref=sources[a][side], dst_ref=landing(a, side),
            send_sem=front_send.at[2 * a + side], recv_sem=edge_recv.at[ix, 2 * (a - 1) + 1 - side],
            device_id={"gx": 0, AXES[a]: me[a] + (1 if side else -1)}, device_id_type=MESH,
        )

    def raw_to_front():
        return pltpu.make_async_remote_copy(
            src_ref=vols.at[ix], dst_ref=vols.at[ix], send_sem=front_send.at[0], recv_sem=raw_recv.at[ix, 0],
            device_id={"gx": 0}, device_id_type=MESH,
        )

    def last_to_front():
        k = raw_from - 1
        return pltpu.make_async_remote_copy(
            src_ref=vols.at[k, depth - 1], dst_ref=vols.at[k, depth - 1],
            send_sem=front_send.at[0], recv_sem=raw_recv.at[k, 0],
            device_id={"gx": 0}, device_id_type=MESH,
        )

    def frame_to_front():
        return pltpu.make_async_remote_copy(
            src_ref=frames.at[ix], dst_ref=frames.at[ix], send_sem=front_send.at[1], recv_sem=raw_recv.at[ix, 1],
            device_id={"gx": 0}, device_id_type=MESH,
        )

    loads[0].wait()

    @pl.when(has_lower[0])
    def _():
        halo_copy(0, 0).start()

    for load in loads[4:]:
        load.wait()

    def send_raw(when):
        @pl.when(when & (ix > 0) & (ix == raw_from - 1) & (raw_from < n))
        def _():
            last_to_front().start()

        @pl.when(when & is_raw)
        def _():
            raw_to_front().start()

    at_first = me[1] + me[2] == 0
    send_raw(at_first)
    vol3 = vols[ix]
    vol = vol3.reshape(depth * rows, lanes)

    def send_lower(a):
        @pl.when(wants_edge(a, 0))
        def _():
            edge_to_front(a, 0).start()

        @pl.when(has_lower[a])
        def _():
            halo_copy(a, 0).start()

    send_lower(1)
    first = jnp.zeros((8, lanes), jnp.int32)
    last = jnp.zeros((8, lanes), jnp.int32)
    for v in range(depth * per):
        piece = vol[v * 8:(v + 1) * 8]
        to_last = (2 * v + 1) % lanes
        to_first = (2 * v - 1) % lanes
        last = jnp.where(lane == 2 * v, pltpu.roll(piece, to_last, 1) if to_last else piece, last)
        first = jnp.where(lane == to_first, pltpu.roll(piece, to_first, 1) if to_first else piece, first)
    zedge[0] = first
    zedge[1] = last
    send_lower(2)
    send_raw(jnp.logical_not(at_first))
    loads[2].wait()
    frames[ix] = jnp.where(
        line == 0,
        ((lane >= foot_ref[0, 0, 0, 2]) & (lane < foot_ref[0, 0, 0, 3])).astype(jnp.int32),
        jnp.where(line == 1, foot_ref[0, 0, 0, 0], foot_ref[0, 0, 0, 1]),
    )

    @pl.when(is_raw)
    def _():
        frame_to_front().start()

    for a in (0, 1, 2):
        @pl.when(has_upper[a])
        def _():
            pl.semaphore_wait(ready.at[a], 1)
            halo_copy(a, 1).start()
    for a in (2, 1):
        @pl.when(wants_edge(a, 1))
        def _():
            edge_to_front(a, 1).start()

    loads[1].wait()

    def inside(b):
        frame = frames[b]
        return (frame[0:1] > 0) & (row_no >= frame[1:2]) & (row_no < frame[2:3])

    def prepare(b):
        transmit = jnp.ones((rows, lanes), jnp.float32)
        d3 = []
        for x in range(depth):
            found = lookup(table_ref, vols[b, x], lanes)
            d3.append(found[3])
            dens[b * depth + x + 1] = d3[x]
            sample = 1.0 - jnp.exp(-extent * d3[x])
            weight = transmit * sample
            transmit = transmit * (1.0 - sample)
            for c in range(3):
                wemit[b, c, x] = weight * found[c]
        alphas[b] = jnp.where(inside(b), 1.0 - transmit, 0.0)
        for x in range(depth):
            d = d3[x]
            up = jnp.where(row_no == 0, 0.0, pltpu.roll(d, 1, 0))
            down = jnp.where(row_no == rows - 1, 0.0, pltpu.roll(d, rows - 1, 0))
            inner[b, 0, x] = 0.5 * (down - up)
            left = jnp.where(lane_no == 0, 0.0, pltpu.roll(d, 1, 1))
            right = jnp.where(lane_no == lanes - 1, 0.0, pltpu.roll(d, lanes - 1, 1))
            inner[b, 1, x] = 0.5 * (right - left)

    half = [
        [jnp.where(has_lower[a], 0.5, 0.0), jnp.where(has_upper[a], 0.5, 0.0)] for a in range(3)
    ]
    even = (lane & 1) == 0
    on_side = (lane == 0) | (lane == lanes - 1)

    def sides_of(b):
        ints = jnp.where(even, zh[b, 0], zh[b, 1])
        return jnp.where(even, -half[2][0], half[2][1]) * lookup(table_ref[3:4, :], ints, lanes)[0]

    def shade(b, span, sides=None):
        sides = sides_of(b) if sides is None else sides
        opacity = table_ref[3:4, :]
        half_up = half[1][0] * lookup(opacity, yh[b, 0], lanes)[0]
        half_down = half[1][1] * lookup(opacity, yh[b, 1], lanes)[0]
        colour = [[None] * per for _ in range(3)]
        for x in span:
            for h in range(per):
                at = pl.ds(h * 8, 8)
                v = x * per + h
                g_x = 0.5 * (dens[b * depth + x + 2, at, :] - dens[b * depth + x, at, :])
                g_y = inner[b, 0, x, at, :]
                if h == 0:
                    g_y = jnp.where(line == 0, g_y - half_up[x:x + 1, :], g_y)
                if h == per - 1:
                    g_y = jnp.where(line == 7, g_y + half_down[x:x + 1, :], g_y)
                side = pltpu.roll(sides, lanes - 2 * v, 1) if v else sides
                g_z = inner[b, 1, x, at, :]
                g_z = jnp.where(on_side, g_z + side, g_z)
                facing = jnp.abs(g_x * LIGHT[0] + g_y * LIGHT[1] + g_z * LIGHT[2]) * lax.rsqrt(
                    1.0 + (g_x * g_x + g_y * g_y + g_z * g_z)
                )
                lit = 0.35 + 0.65 * facing
                for c in range(3):
                    term = wemit[b, c, x, at, :] * lit
                    colour[c][h] = term if colour[c][h] is None else colour[c][h] + term
        return [jnp.where(inside(b), jnp.concatenate(c, axis=0), 0.0) for c in colour]

    prepare(ix)

    def image_copy(buf, off, s_sem, r_sem):
        return pltpu.make_async_remote_copy(
            src_ref=buf.at[ix], dst_ref=buf.at[ix], send_sem=s_sem.at[off], recv_sem=r_sem.at[off],
            device_id={"gx": lax.rem(ix + off, n)}, device_id_type=MESH,
        )

    def for_images(act):
        for far in range(n - 1, 0, -1):
            @pl.when(ix + far < n)
            def _():
                act(far)

            @pl.when((ix - far >= 1) | ((ix == far) & (far < raw_from)))
            def _():
                act(n - far)

    @pl.when(ix < n - 2)
    def _():
        pl.semaphore_wait(far_ready, n - 2 - ix)
    for_images(lambda off: image_copy(alphas, off, a_send, a_recv).start())

    def await_halo(a):
        @pl.when(has_lower[a])
        def _():
            halo_copy(a, 1).wait_recv()

        @pl.when(has_upper[a])
        def _():
            halo_copy(a, 0).wait_recv()

    await_halo(0)
    opacity = table_ref[3:4, :]
    dens[ix * depth] = 2.0 * half[0][0] * lookup(opacity, xh[0], lanes)[0]
    dens[ix * depth + depth + 1] = 2.0 * half[0][1] * lookup(opacity, xh[1], lanes)[0]
    await_halo(2)
    own_sides = sides_of(ix)
    await_halo(1)
    own = shade(ix, range(depth), own_sides)
    for c in range(3):
        colours[ix, c] = own[c]
    for_images(lambda off: image_copy(colours, off, c_send, c_recv).start())
    loads[3].wait()

    @pl.when((ix == 0) & (raw_from < n))
    def _():
        def step(b, carry):
            for which in range(2):
                pltpu.make_async_remote_copy(
                    src_ref=(vols, frames)[which].at[b], dst_ref=(vols, frames)[which].at[b],
                    send_sem=front_send.at[which], recv_sem=raw_recv.at[b, which],
                    device_id={"gx": 1}, device_id_type=MESH,
                ).wait_recv()
            prepare(b)
            for a, halo in ((1, yh), (2, zh)):
                for side, there in ((0, has_lower[a]), (1, has_upper[a])):
                    @pl.when(there)
                    def _():
                        pltpu.make_async_remote_copy(
                            src_ref=halo.at[b, side], dst_ref=halo.at[b, side],
                            send_sem=front_send.at[0], recv_sem=edge_recv.at[b, 2 * (a - 1) + side],
                            device_id={"gx": 1}, device_id_type=MESH,
                        ).wait_recv()

            def cast(span, follows):
                got = shade(b, span)
                rest = shade(b - 1, (depth - 1,)) if follows else None
                for c in range(3):
                    colours[b, c] = got[c]
                    if follows:
                        colours[b - 1, c] = colours[b - 1, c] + rest[c]

            for is_last, span in ((False, range(depth - 1)), (True, range(depth))):
                for follows in (False, True):
                    @pl.when(((b == n - 1) == is_last) & ((b > raw_from) == follows))
                    def _():
                        cast(span, follows)
            return carry

        dens[n * depth + 1] = jnp.zeros((rows, lanes), jnp.float32)

        @pl.when(raw_from > 1)
        def _():
            pltpu.make_async_remote_copy(
                src_ref=vols.at[raw_from - 1, depth - 1], dst_ref=vols.at[raw_from - 1, depth - 1],
                send_sem=front_send.at[0], recv_sem=raw_recv.at[raw_from - 1, 0],
                device_id={"gx": 1}, device_id_type=MESH,
            ).wait_recv()
            dens[raw_from * depth] = lookup(opacity, vols[raw_from - 1, depth - 1], lanes)[0]
        lax.fori_loop(raw_from, n, step, 0)

    for off in range(1, n):
        @pl.when((ix > 0) | (n - off < raw_from))
        def _():
            image_copy(alphas, off, a_send, a_recv).wait_recv()

    clear = [1.0 - alphas[b] for b in range(n)]

    def cover(rank):
        seen = jnp.ones((rows, lanes), jnp.float32)
        for b in range(n):
            seen = seen * jnp.where(rank_ref[b] < rank, clear[b], 1.0)
        return seen

    order = [lax.rem(ix + off, n) for off in range(n)]
    covers = [cover(rank_ref[b]) for b in order]
    alpha = covers[0] * alphas[ix]
    for off in range(1, n):
        alpha = alpha + covers[off] * alphas[order[off]]
    out_ref[3] = alpha
    for a in range(3):
        @pl.when(has_lower[a])
        def _():
            halo_copy(a, 0).wait_send()

        @pl.when(has_upper[a])
        def _():
            halo_copy(a, 1).wait_send()
    for a in (1, 2):
        for side in range(2):
            @pl.when(wants_edge(a, side))
            def _():
                edge_to_front(a, side).wait_send()

    @pl.when((ix > 0) & (ix == raw_from - 1) & (raw_from < n))
    def _():
        last_to_front().wait_send()

    @pl.when(is_raw)
    def _():
        frame_to_front().wait_send()
        raw_to_front().wait_send()
    for_images(lambda off: image_copy(alphas, off, a_send, a_recv).wait_send())
    for_images(lambda off: image_copy(colours, off, c_send, c_recv).wait_send())

    total = [covers[0] * colours[ix, c] for c in range(3)]
    for off in range(1, n):
        @pl.when((ix > 0) | (off < raw_from))
        def _():
            image_copy(colours, n - off, c_send, c_recv).wait_recv()
        total = [total[c] + covers[off] * colours[order[off], c] for c in range(3)]
    for c in range(3):
        out_ref[c] = total[c]


def on_device(sizes, volume, transfer_table, depth_rank, footprint):
    depth, rows, lanes = volume.shape
    n = sizes[0]
    vmem = pl.BlockSpec(memory_space=pltpu.VMEM)
    hbm = pl.BlockSpec(memory_space=pl.ANY)
    return pl.pallas_call(
        functools.partial(kernel, sizes),
        out_shape=pltpu.VMEM((4, rows, lanes), jnp.float32),
        in_specs=[hbm] * 4,
        out_specs=vmem,
        scratch_shapes=[
            pltpu.VMEM((n,) + volume.shape, jnp.int32),
            pltpu.VMEM(transfer_table.shape, jnp.float32),
            pltpu.SMEM(depth_rank.shape, jnp.int32),
            pltpu.SMEM(footprint.shape, jnp.int32),
            pltpu.SemaphoreType.DMA((5,)),
            pltpu.VMEM((n, 8, lanes), jnp.int32),
            pltpu.VMEM((2, 8, lanes), jnp.int32),
            pltpu.VMEM((2, rows, lanes), jnp.int32),
            pltpu.VMEM((n, 2, depth, lanes), jnp.int32),
            pltpu.VMEM((n, 2, 8, lanes), jnp.int32),
            pltpu.VMEM((n * depth + 2, rows, lanes), jnp.float32),
            pltpu.VMEM((n, 3, depth, rows, lanes), jnp.float32),
            pltpu.VMEM((n, 2, depth, rows, lanes), jnp.float32),
            pltpu.VMEM((n, rows, lanes), jnp.float32),
            pltpu.VMEM((n, 3, rows, lanes), jnp.float32),
            pltpu.SemaphoreType.REGULAR((3,)),
            pltpu.SemaphoreType.REGULAR,
            pltpu.SemaphoreType.DMA((3, 2)),
            pltpu.SemaphoreType.DMA((3, 2)),
            pltpu.SemaphoreType.DMA((6,)),
            pltpu.SemaphoreType.DMA((n, 2)),
            pltpu.SemaphoreType.DMA((n, 4)),
            pltpu.SemaphoreType.DMA((n,)),
            pltpu.SemaphoreType.DMA((n,)),
            pltpu.SemaphoreType.DMA((n,)),
            pltpu.SemaphoreType.DMA((n,)),
        ],
        compiler_params=pltpu.CompilerParams(collective_id=0, has_side_effects=True),
        name="raycast",
    )(volume, transfer_table, depth_rank, footprint)


def solution(mesh):
    placed = (P("gx", "gy", "gz"), P(), P(), P("gx", "gy", "gz", None))
    sizes = tuple(mesh.shape[a] for a in AXES)
    return jax.shard_map(
        functools.partial(on_device, sizes), mesh=mesh, in_specs=placed,
        out_specs=P(None, "gy", "gz"), check_vma=False,
    )
```
